32 devices in a mesh: dp: 16 (over z, y, x), mp: 2 (over core).
Axes of the slice: x: 2, y: 2, z: 4, core: 2. Of those that a mesh axis runs over, the one named last changes fastest.
Arguments:
- image_tokens: bfloat16 [384, 145, 768], P(('dp', 'mp')), may hold values from -6 to 6
- image_group: int32 [384], P(('dp', 'mp')), may hold values 0 or 1
- image_prenorm: float32 [768], replicated, may hold values from 0.1 to 1.9
- image_qkv: bfloat16 [3, 768, 768], P(None, None, 'mp'), may hold values from -0.21875 to 0.21875
- image_out: bfloat16 [768, 768], P('mp'), may hold values from -0.625 to 0.625
- image_midnorm: float32 [768], replicated, may hold values from 0.1 to 1.9
- image_up: bfloat16 [768, 3072], P(None, 'mp'), may hold values from -0.21875 to 0.21875
- image_down: bfloat16 [3072, 768], P('mp'), may hold values from -0.109375 to 0.109375
- caption_ids: int32 [384, 16], P(('dp', 'mp')), may hold values from 0 to 31999, as said below
- text_tokens: bfloat16 [384, 16, 768], P(('dp', 'mp')), may hold values from -6 to 6
- text_prenorm: float32 [768], replicated, may hold values from 0.1 to 1.9
- text_qkv: bfloat16 [3, 768, 768], P(None, None, 'mp'), may hold values from -0.21875 to 0.21875
- text_out: bfloat16 [768, 768], P('mp'), may hold values from -0.625 to 0.625
- text_midnorm: float32 [768], replicated, may hold values from 0.1 to 1.9
- text_up: bfloat16 [768, 3072], P(None, 'mp'), may hold values from -0.21875 to 0.21875
- text_down: bfloat16 [3072, 768], P('mp'), may hold values from -0.109375 to 0.109375
- logit_scale: float32 [1], replicated, may hold values from 3.7 to 4.4
Outputs:
- loss_mean: float32 [1], replicated
- tokens_grad: float32 [384, 16, 768], P(('dp', 'mp'))
- prenorm_grad: float32 [768], replicated
- qkv_grad: float32 [3, 768, 768], P(None, None, 'mp')
- out_grad: float32 [768, 768], P('mp')
- midnorm_grad: float32 [768], replicated
- up_grad: float32 [768, 3072], P(None, 'mp')
- down_grad: float32 [3072, 768], P('mp')
- scale_grad: float32 [1], replicated
The draws below stay inside these ranges and needn't reach their ends.
Inputs may be any that keep to these rules, and one draw needn't show every extreme that they name: `image_group`: 1 marks a pair whose image has 145 tokens, 0 one whose image has 50; positions past an image's tokens are not part of it. `caption_ids`: 0 is padding; each caption holds 2 or more nonzero ids followed only by zeros.
All inputs are finite; a program needn't handle non-finite values. No bound on the sum of `image_group` on one device may be relied on, other than what follows from the above.
Results may differ from the reference program's by a relative error of at most 0.015.
Values may be sent and summed in bfloat16 or wider, within the bound.
A program may use at most 192 MiB of HBM per device.

```python
import jax
import jax.numpy as jnp
from jax import lax

D = 768
HEADS = 12
HEAD_DIM = 64
FF = 3072
IMG_LEN = 145
SMALL_LEN = 50
TXT_LEN = 16
VOCAB = 32000
PAIR_DEV = 12
PAIRS = 384


def draw_caption_ids(key, part):
    key_len, key_ids, key_pick = jax.random.split(key, 3)
    lengths = jax.random.randint(key_len, (PAIRS, 1), 2, TXT_LEN + 1)
    tokens = jax.random.randint(key_ids, (PAIRS, TXT_LEN), 1, VOCAB)
    positions = jnp.arange(TXT_LEN)[None, :]
    tokens = jnp.where(positions < lengths, tokens, 0)
    chosen = jax.random.randint(key_pick, (), 0, PAIRS)
    tokens = tokens.at[chosen, 0].set(VOCAB - 1)
    return tokens.astype(jnp.int32)


def with_ends(array, own_key, smallest, largest):
    dims = array.shape
    spot = [jax.random.randint(jax.random.fold_in(own_key, axis), (), 0, dims[axis]) for axis in range(len(dims))]
    array = array.at[tuple(spot)].set(smallest)
    longest = dims.index(max(dims))
    spot[longest] = (spot[longest] + 1) % dims[longest]
    return array.at[tuple(spot)].set(largest)


def block_levels(key, extent, pieces, smallest, top_value):
    level = 1.0
    for dim, blocks in pieces:
        draws = jax.random.uniform(jax.random.fold_in(jax.random.fold_in(key, 6), dim), (blocks,), jnp.float32, smallest / len(pieces), top_value / len(pieces))
        level = level * jnp.repeat(jnp.exp(draws), extent[dim] // blocks).reshape((-1,) + (1,) * (len(extent) - 1 - dim))
    return level


def bell_draw(own_key, shape, scale, bound, shards=(), dtype=jnp.bfloat16):
    factor_of = block_levels(own_key, shape, shards, -0.22, 0.18) if shards else 1.0
    drawn = jax.random.normal(own_key, shape, jnp.float32) * scale * factor_of
    return jnp.minimum(jnp.maximum(drawn, -bound), bound).astype(dtype)


def setup_inputs(seed: int = 0) -> dict:
    key_list = jax.random.split(jax.random.key(seed), 18)
    image_tokens = bell_draw(key_list[0], (PAIRS, IMG_LEN, D), 1.0, 6.0, ((0, 32),))
    image_group = with_ends((jax.random.randint(key_list[1], (PAIRS,), 0, 6) < 1).astype(jnp.int32), jax.random.fold_in(key_list[1], 1), 0, 1)
    image_prenorm = jnp.clip(1.0 + 0.18 * jax.random.normal(key_list[2], (D,), jnp.float32), 0.1, 1.9)
    image_qkv = bell_draw(key_list[3], (3, D, D), D ** -0.5, 0.21875, ((2, 2),))
    image_out = bell_draw(key_list[4], (D, D), (D // 8) ** -0.5, 0.625, ((0, 2),))
    image_midnorm = jnp.clip(1.0 + 0.18 * jax.random.normal(key_list[5], (D,), jnp.float32), 0.1, 1.9)
    image_up = bell_draw(key_list[6], (D, FF), D ** -0.5, 0.21875, ((1, 2),))
    image_down = bell_draw(key_list[7], (FF, D), FF ** -0.5, 0.109375, ((0, 2),))
    caption_ids = draw_caption_ids(jax.random.fold_in(key_list[17], 71), 0)
    text_tokens = bell_draw(key_list[9], (PAIRS, TXT_LEN, D), 1.0, 6.0, ((0, 32),))
    text_prenorm = jnp.clip(1.0 + 0.18 * jax.random.normal(key_list[10], (D,), jnp.float32), 0.1, 1.9)
    text_qkv = bell_draw(key_list[11], (3, D, D), D ** -0.5, 0.21875, ((2, 2),))
    text_out = bell_draw(key_list[12], (D, D), (D // 8) ** -0.5, 0.625, ((0, 2),))
    text_midnorm = jnp.clip(1.0 + 0.18 * jax.random.normal(key_list[13], (D,), jnp.float32), 0.1, 1.9)
    text_up = bell_draw(key_list[14], (D, FF), D ** -0.5, 0.21875, ((1, 2),))
    text_down = bell_draw(key_list[15], (FF, D), FF ** -0.5, 0.109375, ((0, 2),))
    logit_scale = jnp.clip(jax.random.uniform(key_list[16], (1,), jnp.float32, 3.7, 4.4), 3.7, 4.4)
    return dict(image_tokens=image_tokens, image_group=image_group, image_prenorm=image_prenorm, image_qkv=image_qkv, image_out=image_out, image_midnorm=image_midnorm, image_up=image_up, image_down=image_down, caption_ids=caption_ids, text_tokens=text_tokens, text_prenorm=text_prenorm, text_qkv=text_qkv, text_out=text_out, text_midnorm=text_midnorm, text_up=text_up, text_down=text_down, logit_scale=logit_scale)


highest = lax.Precision.HIGHEST
epsilon = 1e-06

@jax.custom_vjp
def low(v):
    return lax.optimization_barrier(v.astype(jnp.bfloat16)).astype(jnp.float32)

@jax.custom_vjp
def low_back(v):
    return v

def low_keep(v):
    return (low(v), None)

def low_pass(kept, grad):
    return (grad,)

def back_keep(v):
    return (v, None)

def back_low(kept, grad):
    return (low(grad),)
low.defvjp(low_keep, low_pass)
low_back.defvjp(back_keep, back_low)

def layer_norm(values, norm_gain):
    centre = lax.optimization_barrier(jnp.mean(values, axis=-1, keepdims=True))
    shifted = values - centre
    spread = lax.optimization_barrier(jnp.mean(shifted * shifted, axis=-1, keepdims=True))
    return shifted * lax.rsqrt(spread + epsilon) * norm_gain

def block(inputs, valid_mask, prenorm, qkv_weight, out_weight, midnorm, up_weight, down_weight):
    normed = low(layer_norm(inputs, prenorm))
    project = low(low_back(jnp.einsum('bld,sde->sble', normed, qkv_weight, precision=highest)))
    split_shape = inputs.shape[:2] + (HEADS, HEAD_DIM)
    queries = project[0].reshape(split_shape)
    key_rows = project[1].reshape(split_shape)
    values = project[2].reshape(split_shape)
    scores = jnp.einsum('bqhe,bkhe->bhqk', queries, key_rows, precision=highest) * HEAD_DIM ** (-0.5)
    scores = low_back(jnp.where(valid_mask[:, None, None, :], scores, -1000000000.0))
    weights = low(jax.nn.softmax(scores, axis=-1))
    mixed_heads = low(low_back(jnp.einsum('bhqk,bkhe->bqhe', weights, values, precision=highest))).reshape(inputs.shape)
    attended = low_back(jnp.einsum('bld,de->ble', mixed_heads, out_weight, precision=highest))
    middle = inputs + attended
    normed_two = low(layer_norm(middle, midnorm))
    hidden = low_back(jnp.einsum('bld,df->blf', normed_two, up_weight, precision=highest))
    activated = low(jax.nn.gelu(hidden, approximate=False))
    return middle + low_back(jnp.einsum('blf,fd->bld', activated, down_weight, precision=highest))

def embed(outputs, valid_mask):
    weights = valid_mask.astype(jnp.float32)
    pooled = lax.optimization_barrier(jnp.sum(outputs * weights[:, :, None], axis=1)) / lax.optimization_barrier(jnp.sum(weights, axis=1))[:, None]
    return low(pooled * lax.rsqrt(lax.optimization_barrier(jnp.sum(pooled * pooled, axis=-1, keepdims=True)) + epsilon))

def reference(image_tokens, image_group, image_prenorm, image_qkv, image_out, image_midnorm, image_up, image_down, caption_ids, text_tokens, text_prenorm, text_qkv, text_out, text_midnorm, text_up, text_down, logit_scale):
    positions = jnp.arange(IMG_LEN)
    limits = jnp.where(image_group == 1, IMG_LEN, SMALL_LEN)
    image_valid = positions[None, :] < limits[:, None]
    image_params = (image_prenorm.astype(jnp.float32), image_qkv.astype(jnp.float32), image_out.astype(jnp.float32), image_midnorm.astype(jnp.float32), image_up.astype(jnp.float32), image_down.astype(jnp.float32))

    def image_part(element):
        tokens, valid_mask = element
        return embed(block(tokens.astype(jnp.float32), valid_mask, *image_params), valid_mask)
    groups = PAIRS // PAIR_DEV
    image_embed = lax.map(image_part, (image_tokens.reshape(groups, PAIR_DEV, IMG_LEN, D), image_valid.reshape(groups, PAIR_DEV, IMG_LEN))).reshape(PAIRS, D)
    text_valid = caption_ids != 0
    text_groups = PAIRS // (2 * PAIR_DEV)

    def objective(tokens, prenorm, qkv_weight, out_weight, midnorm, up_weight, down_weight, scale_log):

        def text_part(element):
            caption_rows, valid_mask = element
            return embed(block(caption_rows, valid_mask, prenorm, qkv_weight, out_weight, midnorm, up_weight, down_weight), valid_mask)
        text_embed = lax.map(jax.checkpoint(text_part), (tokens.reshape(text_groups, 2 * PAIR_DEV, TXT_LEN, D), text_valid.reshape(text_groups, 2 * PAIR_DEV, TXT_LEN))).reshape(PAIRS, D)
        cosine = jnp.dot(text_embed, image_embed.T, precision=highest)
        scale_value = jnp.exp(scale_log[0])
        by_rows = low_back(scale_value * cosine)
        by_cols = low_back(scale_value * cosine)
        row_terms = jax.scipy.special.logsumexp(by_rows, axis=1) - jnp.diagonal(by_rows)
        col_terms = jax.scipy.special.logsumexp(by_cols, axis=0) - jnp.diagonal(by_cols)
        return jnp.reshape(0.5 * (jnp.mean(row_terms) + jnp.mean(col_terms)), (1,))
    primals = (text_tokens.astype(jnp.float32), text_prenorm.astype(jnp.float32), text_qkv.astype(jnp.float32), text_out.astype(jnp.float32), text_midnorm.astype(jnp.float32), text_up.astype(jnp.float32), text_down.astype(jnp.float32), logit_scale.astype(jnp.float32))
    loss_mean, pullback = jax.vjp(objective, *primals)
    gradients = pullback(jnp.full((1,), PAIRS, jnp.float32))
    return (loss_mean, gradients[0], gradients[1], gradients[2], gradients[3], gradients[4], gradients[5], gradients[6], gradients[7])
```

```python
import functools

import jax
import jax.numpy as jnp
from jax import lax
from jax.experimental import pallas as pl
from jax.experimental.pallas import tpu as pltpu
from jax.sharding import PartitionSpec as P

HEAD_DIM = 64
SMALL_LEN = 50
EPS = 1e-06
MESH = pl.DeviceIdType.MESH
BF = jnp.bfloat16
F32 = jnp.float32
VMEM_LIMIT = 62 * 1024 * 1024
HIGH = lax.Precision.HIGHEST


def dot(a, b):
    return jnp.dot(a, b, preferred_element_type=F32)


def dot_nt(a, b):
    return lax.dot_general(a, b, (((1,), (1,)), ((), ())), preferred_element_type=F32)


def dot_tn(a, b):
    return lax.dot_general(a, b, (((0,), (0,)), ((), ())), preferred_element_type=F32)


def normed(values):
    centre = jnp.mean(values, axis=-1, keepdims=True)
    shifted = values - centre
    spread = jnp.mean(shifted * shifted, axis=-1, keepdims=True)
    rate = lax.rsqrt(spread + EPS)
    return shifted * rate, rate


def iota(shape, axis):
    return lax.broadcasted_iota(jnp.int32, shape, axis)


def lane_masks():
    low = (iota((1, 128), 1) < 64).astype(F32)
    return low.astype(BF), (1.0 - low).astype(BF)


def stacked(pair):
    low, high = lane_masks()
    return jnp.concatenate([pair * low, pair * high], axis=0)


def halves(both):
    rows = both.shape[0] // 2
    return jnp.where(iota((rows, 128), 1) < 64, both[:rows], both[rows:])


def softmax_of(scores, mask):
    scores = jnp.where(mask, scores * HEAD_DIM ** (-0.5), -1000000000.0)
    shifted = jnp.exp(scores - jnp.max(scores, axis=-1, keepdims=True))
    return shifted * (1.0 / jnp.sum(shifted, axis=-1, keepdims=True))


def embed_of(total):
    return total * lax.rsqrt(jnp.sum(total * total, axis=-1, keepdims=True) + EPS)


def split_dot(left, right):
    top = left.astype(BF)
    rest = (left - top.astype(F32)).astype(BF)
    both = dot(jnp.concatenate([top, rest], axis=0), right)
    return both[: left.shape[0]] + both[left.shape[0] :]


def image_tile(refs, rows, images, length, out_rows):
    (tokens, prenorm, qkv, out, midnorm, up, xs, hs, proj, mixed, pooled_act, pooled_rows) = refs
    count = rows * images
    for k in range(images):
        start = k * rows
        if rows > length:
            whole = length // 16 * 16
            xs[start + whole : start + rows] = jnp.zeros((rows - whole, xs.shape[1]), F32)
            xs[start : start + whole] = tokens[k][0, :whole].astype(F32)
            xs[start + whole : start + length] = tokens[k][0, whole:length].astype(F32)
        else:
            xs[start : start + rows] = tokens[k][0, :rows].astype(F32)
    valid_len = length if rows > length else SMALL_LEN
    span = slice(0, count)
    hs[span] = (normed(xs[span])[0] * prenorm[...]).astype(BF)
    for half in range(2):
        for s in range(3):
            proj[half, s, span] = dot(hs[span], qkv[half][s]).astype(BF)
    block = count // 2
    each = images // 2
    row_of, key_of = iota((2 * block, block), 0) % block, iota((2 * block, block), 1)
    mask = key_of % rows < valid_len
    if each > 1:
        mask = mask & (row_of // rows == key_of // rows)
    width = proj.shape[3]
    for half in range(2):
        for pair in range(width // 128):
            lanes = slice(pair * 128, pair * 128 + 128)
            for b in range(2):
                part = slice(b * block, b * block + block)
                scores = dot_nt(stacked(proj[half, 0, part, lanes]), proj[half, 1, part, lanes])
                weights = softmax_of(scores, mask).astype(BF)
                mixed[half, part, lanes] = halves(dot(weights, proj[half, 2, part, lanes])).astype(BF)
    resid = xs[span] + dot(mixed[0, span], out[0][...]) + dot(mixed[1, span], out[1][...])
    hs[span] = (normed(resid)[0] * midnorm[...]).astype(BF)
    row_at = iota((16, count), 1)
    chosen = ((row_at // rows == iota((16, count), 0)) & (row_at % rows < valid_len)).astype(F32)
    sums = jnp.dot(chosen, resid, precision=HIGH, preferred_element_type=F32)
    for k in range(images):
        pooled_rows[pl.ds(out_rows(k), 1)] = sums[k : k + 1]
    chosen = chosen.astype(BF)
    step = 512
    units = up[0].shape[1]
    for half in range(2):
        for c in range(0, units, step):
            hidden = dot(hs[span], up[half][:, c : c + step])
            act = (0.5 * hidden * (1.0 + lax.erf(hidden * 0.7071067811865476))).astype(BF)
            sums = dot(chosen, act)
            for k in range(images):
                pooled_act[pl.ds(out_rows(k), 1), half * units + c : half * units + c + step] = sums[k : k + 1]


def image_kernel(length, kind, index, target, *refs):
    tokens, rest = refs[:4], refs[4:]
    (prenorm, qkv_a, qkv_b, out_a, out_b, midnorm, up_a, up_b, down_a, down_b, counts, result) = rest[:12]
    xs, hs, proj, mixed, pooled_act, pooled_rows = rest[12:]
    t = pl.program_id(0)
    scratch = (xs, hs, proj, mixed, pooled_act, pooled_rows)
    common = (prenorm, (qkv_a, qkv_b), (out_a, out_b), midnorm, (up_a, up_b)) + scratch

    @pl.when(t == 0)
    def _():
        pooled_act[...] = jnp.zeros_like(pooled_act)
        pooled_rows[...] = jnp.zeros_like(pooled_rows)

    @pl.when(kind[t] == 1)
    def _():
        image_tile((tokens,) + common, 64, 4, length, lambda k: target[4 * t + k])

    @pl.when(kind[t] == 2)
    def _():
        image_tile((tokens,) + common, -(-length // 16) * 16, 2, length, lambda k: target[4 * t + k])

    @pl.when(t == pl.num_programs(0) - 1)
    def _():
        units = down_a.shape[0]
        total = (
            pooled_rows[...]
            + split_dot(pooled_act[:, :units], down_a[...])
            + split_dot(pooled_act[:, units:], down_b[...])
        )
        result[...] = embed_of(total / counts[...]).astype(BF)


def image_embeds(tokens, group, prenorm, qkv, out, midnorm, up, down):
    images, length, width = tokens.shape
    tiles = images // 2 + 1
    large = (group == 1).astype(jnp.int32)
    order = jnp.argsort(large, stable=True).astype(jnp.int32)
    small = images - jnp.sum(large)
    small_tiles = (small + 3) // 4
    large_tiles = (images - small + 1) // 2
    t = jnp.arange(tiles)[:, None]
    k = jnp.arange(4)[None, :]
    is_small = t < small_tiles
    slot = jnp.where(is_small, 4 * t + k, small + 2 * (t - small_tiles) + k)
    good = jnp.where(is_small, slot < small, (slot < images) & (k < 2))
    picked = order[jnp.clip(slot, 0, images - 1)]
    kind = jnp.where(t < small_tiles, 1, jnp.where(t < small_tiles + large_tiles, 2, 0))[:, 0].astype(jnp.int32)
    target = jnp.where(good, picked, 15).reshape(-1).astype(jnp.int32)
    index = picked.reshape(-1).astype(jnp.int32)
    counts = jnp.where(group == 1, length, SMALL_LEN).astype(F32)[:, None]
    counts = jnp.concatenate([counts, jnp.ones((16 - images, 1), F32)])
    wide = up[0].shape[1]
    narrow = qkv[0].shape[2]
    rows = max(256, 2 * (-(-length // 16) * 16))

    def token_spec(slot_at):
        return pl.BlockSpec((1, length, width), lambda i, kind, index, target: (index[4 * i + slot_at], 0, 0))

    def fixed(array):
        zeros = (0,) * array.ndim
        return pl.BlockSpec(array.shape, lambda i, *_: zeros, pipeline_mode=pl.Buffered(1))

    operands = (prenorm[None], qkv[0], qkv[1], out[0], out[1], midnorm[None], up[0], up[1], down[0], down[1], counts)
    return pl.pallas_call(
        functools.partial(image_kernel, length),
        out_shape=jax.ShapeDtypeStruct((16, width), BF),
        grid_spec=pltpu.PrefetchScalarGridSpec(
            num_scalar_prefetch=3,
            grid=(tiles,),
            in_specs=[token_spec(k) for k in range(4)] + [fixed(a) for a in operands],
            out_specs=pl.BlockSpec((16, width), lambda i, *_: (0, 0)),
            scratch_shapes=[
                pltpu.VMEM((rows, width), F32),
                pltpu.VMEM((rows, width), BF),
                pltpu.VMEM((2, 3, rows, narrow), BF),
                pltpu.VMEM((2, rows, narrow), BF),
                pltpu.VMEM((16, 2 * wide), F32),
                pltpu.VMEM((16, width), F32),
            ],
        ),
        compiler_params=pltpu.CompilerParams(vmem_limit_bytes=VMEM_LIMIT),
        cost_estimate=pl.CostEstimate(flops=18 * 10**9, bytes_accessed=20 * 10**6, transcendentals=5 * 10**6),
        name="image_block",
    )(kind, index, target, tokens, tokens, tokens, tokens, *operands)


def text_forward_kernel(
    span, tokens, valid_row, valid_keys, counts, prenorm, qkv_a, qkv_b, out_a, out_b, midnorm, up_a, up_b, down_a, down_b,
    h1, proj, mixed, resid, h2, slope, act_sum, total, embed, act_full,
):
    rows = tokens.shape[0]
    x = tokens[...].astype(F32)
    h1[...] = (normed(x)[0] * prenorm[...]).astype(BF)
    for half, qkv in enumerate((qkv_a, qkv_b)):
        for s in range(3):
            proj[half, s] = dot(h1[...], qkv[s]).astype(BF)
    block = rows // 2
    row_of, key_of = iota((2 * block, block), 0) % block, iota((2 * block, block), 1)
    same = row_of // span == key_of // span
    for half in range(2):
        for pair in range(proj.shape[3] // 128):
            lanes = slice(pair * 128, pair * 128 + 128)
            for b in range(2):
                part = slice(b * block, b * block + block)
                mask = same & (valid_keys[b] > 0.0)
                scores = dot_nt(stacked(proj[half, 0, part, lanes]), proj[half, 1, part, lanes])
                weights = softmax_of(scores, mask).astype(BF)
                mixed[half, part, lanes] = halves(dot(weights, proj[half, 2, part, lanes])).astype(BF)
    middle = x + dot(mixed[0], out_a[...]) + dot(mixed[1], out_b[...])
    resid[...] = middle
    h2[...] = (normed(middle)[0] * midnorm[...]).astype(BF)
    chosen = jnp.where(iota((16, rows), 1) // span == iota((16, rows), 0), valid_row[...], 0.0)
    sums = jnp.dot(chosen, middle, precision=HIGH, preferred_element_type=F32)
    chosen = chosen.astype(BF)
    step = 512
    units = up_a.shape[1]
    for half, up in enumerate((up_a, up_b)):
        for c in range(0, units, step):
            cols = slice(c, c + step)
            hidden = dot(h2[...], up[:, cols])
            cdf = 0.5 * (1.0 + lax.erf(hidden * 0.7071067811865476))
            slope[half, :, cols] = cdf + hidden * 0.3989422804014327 * jnp.exp(-0.5 * hidden * hidden)
            act_full[half, :, cols] = dot(chosen, (hidden * cdf).astype(BF))
    act_sum[...] = act_full[...].astype(BF)
    u = (sums + split_dot(act_full[0], down_a[...]) + split_dot(act_full[1], down_b[...])) / counts[...]
    total[...] = u
    embed[...] = embed_of(u).astype(BF)


def text_backward_kernel(
    span, tokens, valid_keys, valid_col, grad, prenorm, qkv_a, qkv_b, out_a, out_b, midnorm, up_a, up_b, down_a, down_b,
    proj, resid, slope,
    tokens_grad, dhidden, drb, dproj, gains, drow, hold,
):
    rows, width = tokens.shape
    captions = rows // span
    gb = grad[...].astype(BF)
    step = 512
    units = up_a.shape[1]
    for c in range(captions):
        part = slice(c * span, c * span + span)
        drow[part] = grad[c : c + 1] * valid_col[part]
    acc = None
    for half, (up, down) in enumerate(((up_a, down_a), (up_b, down_b))):
        for c in range(0, units, step):
            cols = slice(c, c + step)
            hold[...] = dot_nt(gb, down[cols])
            for i in range(captions):
                part = slice(i * span, i * span + span)
                dhidden[half, part, cols] = (hold[i : i + 1] * (slope[half, part, cols] * valid_col[part])).astype(BF)
        term = dot_nt(dhidden[half], up[...])
        acc = term if acc is None else acc + term
    shape, rate = normed(resid[...])
    gains[1:2] = jnp.sum(acc * shape, axis=0, keepdims=True)
    scaled = acc * midnorm[...]
    drow[...] += rate * (
        scaled - jnp.mean(scaled, axis=-1, keepdims=True) - shape * jnp.mean(scaled * shape, axis=-1, keepdims=True)
    )
    drb[...] = drow[...].astype(BF)
    block = rows // 2
    row_of, key_of = iota((2 * block, block), 0) % block, iota((2 * block, block), 1)
    same = row_of // span == key_of // span
    scale = HEAD_DIM ** (-0.5)
    for half, out in enumerate((out_a, out_b)):
        dmixed = dot_nt(drb[...], out[...]).astype(BF)
        for pair in range(proj.shape[3] // 128):
            lanes = slice(pair * 128, pair * 128 + 128)
            for b in range(2):
                part = slice(b * block, b * block + block)
                mask = same & (valid_keys[b] > 0.0)
                q = stacked(proj[half, 0, part, lanes])
                k = proj[half, 1, part, lanes]
                v = proj[half, 2, part, lanes]
                dm = stacked(dmixed[part, lanes])
                probs = softmax_of(dot_nt(q, k), mask)
                dweights = dot_nt(dm, v)
                ds = (probs * (dweights - jnp.sum(dweights * probs, axis=-1, keepdims=True))).astype(BF)
                dproj[half, 0, part, lanes] = (halves(dot(ds, k)) * scale).astype(BF)
                dproj[half, 1, part, lanes] = (dot_tn(ds, q) * scale).astype(BF)
                dproj[half, 2, part, lanes] = dot_tn(probs.astype(BF), dm).astype(BF)
    acc = None
    for half, qkv in enumerate((qkv_a, qkv_b)):
        for s in range(3):
            term = dot_nt(dproj[half, s], qkv[s])
            acc = term if acc is None else acc + term
    shape, rate = normed(tokens[...].astype(F32))
    gains[0:1] = jnp.sum(acc * shape, axis=0, keepdims=True)
    gains[2:8] = jnp.zeros((6, width), F32)
    scaled = acc * prenorm[...]
    tokens_grad[...] = drow[...] + rate * (
        scaled - jnp.mean(scaled, axis=-1, keepdims=True) - shape * jnp.mean(scaled * shape, axis=-1, keepdims=True)
    )


def local_call(kernel, name, outs, scratch, operands, flops):
    return pl.pallas_call(
        kernel,
        out_shape=[jax.ShapeDtypeStruct(s, d) for s, d in outs],
        in_specs=[pl.BlockSpec(memory_space=pltpu.VMEM)] * len(operands),
        out_specs=[pl.BlockSpec(memory_space=pltpu.VMEM)] * len(outs),
        scratch_shapes=[pltpu.VMEM(s, d) for s, d in scratch],
        compiler_params=pltpu.CompilerParams(vmem_limit_bytes=VMEM_LIMIT),
        cost_estimate=pl.CostEstimate(flops=flops, bytes_accessed=20 * 10**6, transcendentals=10**6),
        name=name,
    )(*operands)


def bit_count(size):
    bits = size.bit_length() - 1
    assert 1 << bits == size, size
    return bits


def my_bit(axis, bit):
    return (lax.axis_index(axis) // (1 << bit)) % 2


def partner_of(axis, bit):
    other = lax.axis_index(axis) + (1 - 2 * my_bit(axis, bit)) * (1 << bit)
    return {axis: other}


def position(order):
    return sum(my_bit(axis, bit) * (1 << at) for at, (axis, bit) in enumerate(order))


def exchange_kernel(plans, *refs):
    count = len(plans)
    ins, outs = refs[:count], refs[count : 2 * count]
    scratch = list(refs[2 * count :])
    send, recv = scratch[0], scratch[1]
    scratch = scratch[2:]
    held = {}
    for c, plan in enumerate(plans):
        if plan[0] == "sum":
            held[c] = scratch[: len(plan[1])]
            scratch = scratch[len(plan[1]) :]
    local = scratch[0]

    steps = sorted({step for plan in plans for step in plan[1]})
    barrier = pltpu.get_barrier_semaphore()
    for axis, bit in steps:
        pl.semaphore_signal(barrier, inc=1, device_id=partner_of(axis, bit), device_id_type=MESH)
    pl.semaphore_wait(barrier, len(steps))

    started = []

    def copy(c, at, src, dst, axis, bit):
        made = pltpu.make_async_remote_copy(
            src_ref=src,
            dst_ref=dst,
            send_sem=send.at[c, at],
            recv_sem=recv.at[c, at],
            device_id=partner_of(axis, bit),
            device_id_type=MESH,
        )
        made.start()
        started.append(made)
        return made

    flight = {}
    region = {}

    for c, plan in enumerate(plans):
        if plan[0] == "gather":
            pos = position(plan[1])
            own = pltpu.make_async_copy(ins[c], outs[c].at[pos], local.at[c])
            own.start()
            own.wait()
            region[c] = pos

    def start_gather(c, at):
        order = plans[c][1]
        axis, bit = order[at]
        size = 1 << at
        piece = outs[c].at[pl.ds(region[c], size)]
        flight[c] = copy(c, plans[c][2] + at, piece, piece, axis, bit)

    def end_gather(c, at):
        order = plans[c][1]
        axis, bit = order[at]
        flight[c].wait_recv()
        region[c] = region[c] - my_bit(axis, bit) * (1 << at)

    def start_sum(c, at):
        order = plans[c][1]
        axis, bit = order[at]
        half = 1 << (len(order) - 1 - at)
        away = (1 - my_bit(axis, bit)) * half
        source = ins[c] if at == 0 else held[c][at - 1]
        flight[c] = copy(c, at, source.at[pl.ds(away, half)], held[c][at], axis, bit)

    def end_sum(c, at):
        order = plans[c][1]
        axis, bit = order[at]
        half = 1 << (len(order) - 1 - at)
        kept = my_bit(axis, bit) * half
        flight[c].wait_recv()
        arrived = held[c][at]
        source = ins[c] if at == 0 else held[c][at - 1]
        last = at == len(order) - 1
        if last:
            pos = sum(my_bit(a, b) * (1 << (len(order) - 1 - i)) for i, (a, b) in enumerate(order))
            region[c] = pos

        def add(i, carry):
            value = (source[kept + i].astype(F32) + arrived[i].astype(F32)).astype(outs[c].dtype)
            if last:
                outs[c][region[c]] = value
            else:
                arrived[i] = value
            return carry

        lax.fori_loop(0, half, add, 0)

    depth = max(len(p[1]) for p in plans)
    order_of = list(range(count))
    for c in order_of:
        if plans[c][0] == "sum":
            start_sum(c, 0)
        else:
            start_gather(c, 0)
    for at in range(depth):
        for c in order_of:
            kind, order = plans[c][0], plans[c][1]
            if at >= len(order):
                continue
            if kind == "sum":
                end_sum(c, at)
                if at + 1 < len(order):
                    start_sum(c, at + 1)
            else:
                end_gather(c, at)
                if at + 1 < len(order):
                    start_gather(c, at + 1)
    summed = [c for c in order_of if plans[c][0] == "sum"]
    if summed:
        def start_back(c, at):
            order = plans[c][1]
            axis, bit = order[len(order) - 1 - at]
            size = 1 << at
            piece = outs[c].at[pl.ds(region[c], size)]
            flight[c] = copy(c, len(order) + at, piece, piece, axis, bit)

        def end_back(c, at):
            order = plans[c][1]
            axis, bit = order[len(order) - 1 - at]
            flight[c].wait_recv()
            region[c] = region[c] - my_bit(axis, bit) * (1 << at)

        for c in summed:
            start_back(c, 0)
        bits = len(plans[summed[0]][1])
        for at in range(bits):
            for c in summed:
                end_back(c, at)
                if at + 1 < bits:
                    start_back(c, at + 1)
    for made in started:
        made.wait_send()


def exchange(name, collective_id, sums, gathers):
    plans = [("sum", tuple(order), 0) for _, order in sums]
    plans += [("gather", tuple(order), 0) for _, order in gathers]
    operands = [a for a, _ in sums] + [a for a, _ in gathers]
    shapes = [jax.ShapeDtypeStruct(a.shape, a.dtype) for a, _ in sums]
    shapes += [jax.ShapeDtypeStruct((1 << len(order),) + a.shape, a.dtype) for a, order in gathers]
    most = max(2 * len(p[1]) if p[0] == "sum" else len(p[1]) for p in plans)
    scratch = [pltpu.SemaphoreType.DMA((len(plans), most)), pltpu.SemaphoreType.DMA((len(plans), most))]
    for a, order in sums:
        n = a.shape[0]
        for at in range(len(order)):
            scratch.append(pltpu.VMEM((n >> (at + 1),) + a.shape[1:], a.dtype))
    scratch.append(pltpu.SemaphoreType.DMA((len(plans),)))
    return pl.pallas_call(
        functools.partial(exchange_kernel, tuple(plans)),
        out_shape=shapes,
        in_specs=[pl.BlockSpec(memory_space=pltpu.VMEM)] * len(operands),
        out_specs=[pl.BlockSpec(memory_space=pltpu.VMEM)] * len(shapes),
        scratch_shapes=scratch,
        compiler_params=pltpu.CompilerParams(
            collective_id=collective_id, has_side_effects=True, vmem_limit_bytes=VMEM_LIMIT
        ),
        name=name,
    )(*operands)


def log_total(values, axis):
    largest = jnp.max(values, axis=axis, keepdims=True)
    return largest + jnp.log(jnp.sum(jnp.exp(values - largest), axis=axis, keepdims=True))


def shards(
    dp_size, image_tokens, image_group, image_prenorm, image_qkv, image_out, image_midnorm, image_up, image_down,
    caption_ids, text_tokens, text_prenorm, text_qkv, text_out, text_midnorm, text_up, text_down, logit_scale,
):
    swap = functools.partial(lax.ppermute, axis_name="mp", perm=[(0, 1), (1, 0)])
    bits = bit_count(dp_size)
    far_first = [("dp", b) for b in reversed(range(bits))]
    x_first = [("dp", b) for b in range(bits)]
    y_first = [("dp", b) for b in [1, 0] + list(range(2, bits))]
    pairs, span = caption_ids.shape
    width = text_tokens.shape[2]
    rows = pairs * span
    narrow = text_qkv.shape[2]
    wide = text_up.shape[1]

    t_qkv = (text_qkv, swap(text_qkv))
    t_out = (text_out, swap(text_out))
    t_up = (text_up, swap(text_up))
    t_down = (text_down, swap(text_down))
    i_qkv = (image_qkv, swap(image_qkv))
    i_out = (image_out, swap(image_out))
    i_up = (image_up, swap(image_up))
    i_down = (image_down, swap(image_down))

    valid = (caption_ids != 0).astype(F32)
    counts = jnp.concatenate([jnp.sum(valid, axis=1, keepdims=True), jnp.ones((16 - pairs, 1), F32)])
    tokens = text_tokens.reshape(rows, width)
    valid_keys = valid.reshape(2, 1, rows // 2)
    weights = (text_prenorm[None],) + t_qkv + t_out + (text_midnorm[None],) + t_up + t_down
    h1, proj, mixed, resid, h2, slope, act_sum, total, text_embed = local_call(
        functools.partial(text_forward_kernel, span),
        "text_forward",
        [
            ((rows, width), BF),
            ((2, 3, rows, narrow), BF),
            ((2, rows, narrow), BF),
            ((rows, width), F32),
            ((rows, width), BF),
            ((2, rows, wide), F32),
            ((2, 16, wide), BF),
            ((16, width), F32),
            ((16, width), BF),
        ],
        [((2, 16, wide), F32)],
        (tokens, valid.reshape(1, rows), valid_keys, counts) + weights,
        3 * 10**9,
    )
    first = lax.axis_index("mp") == 0

    def in_order(mine, theirs):
        return jnp.where(first, jnp.concatenate([mine, theirs]), jnp.concatenate([theirs, mine]))

    act_pair = in_order(act_sum[0, :pairs], swap(act_sum[1, :pairs]))
    h1_both = jnp.concatenate([h1, swap(h1)])
    h2_both = jnp.concatenate([h2, swap(h2)])
    mixed_both = jnp.concatenate([mixed[0], swap(mixed[1])])

    image_embed = image_embeds(
        image_tokens, image_group, image_prenorm, i_qkv, i_out, image_midnorm, i_up, i_down
    )

    embed_order = far_first + [("mp", 0)]
    every_text, every_image = exchange(
        "embeds", 1, [], [(text_embed[:pairs], embed_order), (image_embed[:pairs], embed_order)]
    )
    every_text = every_text.reshape(-1, width)
    every_image = every_image.reshape(-1, width)
    all_pairs = every_text.shape[0]
    scale_value = jnp.exp(logit_scale[0])
    logits = scale_value * dot_nt(every_text, every_image)
    here = (jnp.arange(all_pairs)[:, None] == jnp.arange(all_pairs)[None, :]).astype(F32)
    row_total = log_total(logits, 1)
    col_total = log_total(logits, 0)
    on_diagonal = jnp.sum(logits * here)
    loss_mean = jnp.reshape(0.5 * (jnp.sum(row_total) + jnp.sum(col_total) - 2.0 * on_diagonal) / all_pairs, (1,))
    both = (0.5 * (jnp.exp(logits - row_total) - here)).astype(BF).astype(F32) + (
        0.5 * (jnp.exp(logits - col_total) - here)
    ).astype(BF).astype(F32)
    scale_grad = jnp.reshape(jnp.sum(both * logits), (1,))
    start = position(embed_order) * pairs
    own_logits = lax.dynamic_slice_in_dim(logits, start, pairs, 0)
    own_here = lax.dynamic_slice_in_dim(here, start, pairs, 0)
    own_total = lax.dynamic_slice_in_dim(row_total, start, pairs, 0)
    grow = (0.5 * (jnp.exp(own_logits - own_total) - own_here)).astype(BF)
    gcol = (0.5 * (jnp.exp(own_logits - col_total) - own_here)).astype(BF)
    dembed = scale_value * (dot(grow, every_image) + dot(gcol, every_image))
    u = total[:pairs]
    rate = lax.rsqrt(jnp.sum(u * u, axis=1, keepdims=True) + EPS)
    grad = (rate * dembed - rate**3 * u * jnp.sum(u * dembed, axis=1, keepdims=True)) / counts[:pairs]
    grad_rows = jnp.concatenate([grad, jnp.zeros((16 - pairs, width), F32)])

    tokens_grad, dhidden, drb, dproj, gains = local_call(
        functools.partial(text_backward_kernel, span),
        "text_backward",
        [
            ((rows, width), F32),
            ((2, rows, wide), BF),
            ((rows, width), BF),
            ((2, 3, rows, narrow), BF),
            ((8, width), F32),
        ],
        [((rows, width), F32), ((16, 512), F32)],
        (tokens, valid_keys, valid.reshape(rows, 1), grad_rows) + weights + (proj, resid, slope),
        4 * 10**9,
    )
    dh_both = jnp.concatenate([dhidden[0], swap(dhidden[1])])
    drb_both = jnp.concatenate([drb, swap(drb)])
    dproj_both = jnp.concatenate([dproj[0], swap(dproj[1])], axis=1)
    gains = gains + swap(gains)

    def split(array):
        return array.astype(BF).reshape(dp_size, array.shape[0] // dp_size, array.shape[1])

    up_grad = [split(dot_tn(h2_both, dh_both[:, : wide // 2])), split(dot_tn(h2_both, dh_both[:, wide // 2 :]))]
    qkv_grad = [split(dot_tn(h1_both, dproj_both[s])) for s in range(3)]
    out_grad = split(dot_tn(mixed_both, drb_both))
    sums = [
        (up_grad[0], x_first), (up_grad[1], y_first), (qkv_grad[0], x_first), (qkv_grad[1], y_first),
        (qkv_grad[2], x_first), (out_grad, y_first),
    ]
    gathers = [(grad.astype(BF), [("mp", 0)] + far_first), (act_pair, far_first), (gains, far_first)]
    up_x, up_y, q_sum, k_sum, v_sum, out_sum, every_grad, every_act, every_gain = exchange(
        "gradients", 2, sums, gathers
    )

    def joined(array):
        return array.reshape(-1, array.shape[2])

    down_grad = dot_tn(joined(every_act), joined(every_grad))
    up_total = jnp.concatenate([joined(up_x), joined(up_y)], axis=1).astype(F32)
    qkv_total = jnp.stack([joined(q_sum), joined(k_sum), joined(v_sum)]).astype(F32)
    gain_total = jnp.sum(every_gain, axis=0)
    return (
        loss_mean,
        tokens_grad.reshape(text_tokens.shape),
        gain_total[0],
        qkv_total,
        joined(out_sum).astype(F32),
        gain_total[1],
        up_total,
        down_grad,
        scale_grad,
    )


def solution(mesh):
    both = ("dp", "mp")
    in_specs = (
        P(both, None, None), P(both), P(), P(None, None, "mp"), P("mp", None), P(), P(None, "mp"), P("mp", None),
        P(both, None), P(both, None, None), P(), P(None, None, "mp"), P("mp", None), P(), P(None, "mp"),
        P("mp", None), P(),
    )
    out_specs = (
        P(), P(both, None, None), P(), P(None, None, "mp"), P("mp", None), P(), P(None, "mp"), P("mp", None), P(),
    )
    step = functools.partial(shards, mesh.shape["dp"])
    return jax.shard_map(step, mesh=mesh, in_specs=in_specs, out_specs=out_specs, check_vma=False)
```
